8 devices in a mesh: dp: 2 (over y, z), tp: 4 (over x, core).
Axes of the slice: x: 2, y: 2, z: 1, core: 2. Of those that a mesh axis runs over, the one named last changes fastest.
Arguments:
- x: bfloat16 [2048, 4096], P(('dp', 'tp')), parts along dimension 0
- w_gate: bfloat16 [4096, 12800], P(None, 'tp')
- w_up: bfloat16 [4096, 12800], P(None, 'tp')
- w_down: bfloat16 [12800, 4096], P('tp')
Outputs:
- output: bfloat16 [2048, 4096], P(('dp', 'tp')), parts along dimension 0
There are 2 independent parts. The reference program is written for one: setup_inputs(seed, part) draws one part's arguments, and reference() takes and returns one part's arrays. A program takes and returns all parts, laid end to end along the dimension named above; an argument that names none is the same for every part.
All inputs are finite; a program needn't handle non-finite values.
Results may differ from the reference program's by a relative error of at most 0.016.
Values are sent between devices in bfloat16 or wider.
A program may use at most 2 GiB of HBM per device.

```python
import jax
import jax.numpy as jnp

ROWS = 1024
D = 4096
FF = 12800


def setup_inputs(seed: int = 0, part: int = 0) -> dict:
    kx, kg, ku, kd = jax.random.split(jax.random.key(seed), 4)
    drawn = {
        "x": jax.random.normal(jax.random.fold_in(kx, part), (ROWS, D), jnp.float32),
        "w_gate": jax.random.normal(kg, (D, FF), jnp.float32) * D**-0.5,
        "w_up": jax.random.normal(ku, (D, FF), jnp.float32) * D**-0.5,
        "w_down": jax.random.normal(kd, (FF, D), jnp.float32) * FF**-0.5,
    }
    return {k: v.astype(jnp.bfloat16) for k, v in drawn.items()}


def reference(x, w_gate, w_up, w_down):
    gate = jnp.dot(x, w_gate, preferred_element_type=jnp.float32)
    up = jnp.dot(x, w_up, preferred_element_type=jnp.float32)
    hidden = (jax.nn.silu(gate) * up).astype(jnp.bfloat16)
    return jnp.dot(hidden, w_down, preferred_element_type=jnp.float32).astype(jnp.bfloat16)
```

```python
import jax
import jax.numpy as jnp
from jax import lax
from jax.experimental import pallas as pl
from jax.experimental.pallas import tpu as pltpu
from jax.sharding import PartitionSpec as P

D = 4096
F = 3200
ROWS = 256
HALF = ROWS // 2
PIECES = 4
PIECE = HALF // PIECES
TA = 256
TB = 512
REM = F - 12 * TA
MESH = pl.DeviceIdType.MESH
BF16 = jnp.bfloat16
F32 = jnp.float32


def kernel(x_hbm, wg, wu, wd, y_hbm,
           xs, h, wr, wc, wrem, snd, o1recv, rrecv, icist, rsrecv, own,
           ring_sem, cache_sem, rem_sem, px_send, px_recv, ownx_sem,
           ag_send, ag_recv, fwd_send, fwd_recv, snd_sem, o1_sem, rr_sem,
           ici_send, rs_sem, out_sem):
    me = lax.axis_index("tp")
    cp = lax.rem(me, 2)
    partner = me + 1 - 2 * cp
    mirror = lax.rem(me + 2, 4)
    far = mirror - cp

    def remote(src, dst, ssem, rsem, dev):
        return pltpu.make_async_remote_copy(
            src_ref=src, dst_ref=dst, send_sem=ssem, recv_sem=rsem,
            device_id={"tp": dev}, device_id_type=MESH)

    def a_copies(t, dst, sems, width):
        cols = pl.ds(t * TA, width)
        return [
            pltpu.make_async_copy(wg.at[:, cols], dst.at[:, pl.ds(0, width)], sems.at[0]),
            pltpu.make_async_copy(wu.at[:, cols], dst.at[:, pl.ds(width, width)], sems.at[1]),
        ]

    def tile_of(i, q):
        return 2 * i + (1 - cp if q == 0 else cp)

    def ring_a(s, b):
        return [c for q in range(2) for c in a_copies(3 * b + q, wr.at[s, q], ring_sem.at[s, q], TA)]

    def ring_b(s, i):
        out_ = []
        for q in range(2):
            cols = pl.ds(pl.multiple_of(tile_of(i, q) * TB, TB), TB)
            out_.append(pltpu.make_async_copy(wd.at[:, cols], wr.at[s, q, pl.ds(0, F), :], ring_sem.at[s, q, 0]))
        return out_

    def cache(b):
        return a_copies(3 * b + 2, wc.at[b], cache_sem.at[b], TA)

    def rem_copies():
        return a_copies(12, wrem, rem_sem, REM)

    def start(copies):
        for c in copies:
            c.start()

    def wait(copies):
        for c in copies:
            c.wait()

    def px():
        return remote(x_hbm, xs.at[0], px_send, px_recv, partner)

    def ag(k, p):
        return remote(x_hbm.at[pl.ds(k * HALF + p * PIECE, PIECE)],
                      xs.at[1 + k, pl.ds(pl.multiple_of(cp * HALF + p * PIECE, PIECE), PIECE)],
                      ag_send.at[k, p], ag_recv.at[k, p], mirror)

    def fwd(k, p):
        rows = pl.ds(pl.multiple_of(cp * HALF + p * PIECE, PIECE), PIECE)
        return remote(xs.at[1 + k, rows], xs.at[1 + k, rows], fwd_send.at[k, p], fwd_recv.at[k, p], partner)

    def o1_copy(j):
        return remote(snd.at[j], o1recv.at[j], snd_sem.at[j], o1_sem.at[j], partner)

    def rr_copy(k, i):
        return remote(snd.at[4 * k + i], rrecv.at[k, i], snd_sem.at[4 * k + i], rr_sem.at[k, i], partner)

    def rs_copy(k, i, r):
        j = tile_of(i, 1)
        return remote(icist.at[k, i, pl.ds(r * HALF, HALF), :],
                      rsrecv.at[j, pl.ds(pl.multiple_of(k * HALF, HALF), HALF), :],
                      ici_send.at[k, i, r], rs_sem.at[k, j], far + r)

    def out_copy(slot, j):
        return pltpu.make_async_copy(
            snd.at[slot], y_hbm.at[:, pl.ds(pl.multiple_of(j * TB, TB), TB)], out_sem.at[slot])

    def ownx():
        return pltpu.make_async_copy(x_hbm, xs.at[0], ownx_sem)

    start(ring_a(0, 0))
    start(cache(0))
    start(ring_a(1, 1))
    start(cache(1))

    barrier = pltpu.get_barrier_semaphore()
    for other in (partner, mirror, mirror + 1 - 2 * cp):
        pl.semaphore_signal(barrier, inc=1, device_id={"tp": other}, device_id_type=MESH)
    pl.semaphore_wait(barrier, 3)

    px().start()
    for k in range(2):
        for p in range(PIECES):
            ag(k, p).start()
    start(cache(2))
    start(cache(3))
    start(rem_copies())

    def finish(k, i, buf):
        rr_copy(k, i).wait_recv()
        icist[k, i] = (own[buf] + rrecv[k, i].astype(F32)).astype(BF16)
        for r in range(2):
            rs_copy(k, i, r).start()

    def glu(gu, width):
        g = gu[:, :width]
        return (g * jax.nn.sigmoid(g) * gu[:, width:]).astype(BF16)

    def chunk(c, carry):
        xi = lax.rem(c, 3)

        @pl.when(c == 0)
        def _():
            px().wait_recv()

        @pl.when(c == 1)
        def _():
            ownx().start()
            for p in range(PIECES):
                fwd(0, p).wait_recv()

        @pl.when(c == 2)
        def _():
            for p in range(PIECES):
                fwd(1, p).wait_recv()

        @pl.when(c == 3)
        def _():
            ownx().wait()

        def forward(p):
            for k in range(2):
                @pl.when(c == k)
                def _():
                    ag(k, p).wait_recv()
                    fwd(k, p).start()

        for b in range(4):
            if b == 1:
                forward(0)
                for k in range(2):
                    @pl.when(c == 2 + k)
                    def _():
                        finish(k, 3, 1)
            if b == 3:
                forward(1)
            s = lax.rem(c * 8 + b, 3)
            wait(ring_a(s, b))

            @pl.when(c == 0)
            def _():
                wait(cache(b))
                if b == 3:
                    wait(rem_copies())

            s2 = lax.rem(c * 8 + b + 2, 3)
            start(ring_a(s2, b + 2) if b + 2 < 4 else ring_b(s2, b + 2 - 4))
            for q in range(3):
                w = wr[s, q] if q < 2 else wc[b]
                gu = jnp.dot(xs[xi], w, preferred_element_type=F32)
                h[:, (3 * b + q) * TA:(3 * b + q + 1) * TA] = glu(gu, TA)
            if b == 3:
                gu = jnp.dot(xs[xi], wrem[...], preferred_element_type=F32)
                h[:, 12 * TA:] = glu(gu, REM)
        forward(2)

        def ring_step(i):
            g = c * 8 + 4 + i
            s = lax.rem(g, 3)
            wait(ring_b(s, i))
            s2 = lax.rem(g + 2, 3)

            @pl.when(i < 2)
            def _():
                start(ring_b(s2, i + 2))

            for b in range(2):
                @pl.when((i == 2 + b) & (c < 3))
                def _():
                    start(ring_a(s2, b))
            return s

        def down(s, q):
            return jnp.dot(h[...], wr[s, q, pl.ds(0, F), :], preferred_element_type=F32)

        @pl.when(c == 0)
        def _():
            def step(i, carry):
                @pl.when(i == 3)
                def _():
                    forward(3)
                s = ring_step(i)
                for q in range(2):
                    snd[tile_of(i, q)] = down(s, q).astype(BF16)
                for q in range(2):
                    o1_copy(tile_of(i, q)).start()
                return carry
            lax.fori_loop(0, 4, step, 0)

        @pl.when((c == 1) | (c == 2))
        def _():
            k = c - 1

            def step(i, carry):
                @pl.when((i == 3) & (c == 1))
                def _():
                    forward(3)
                s = ring_step(i)
                o1_copy(4 * k + i).wait_send()
                snd[4 * k + i] = down(s, 0).astype(BF16)
                own[lax.rem(i, 2)] = down(s, 1)
                rr_copy(k, i).start()

                @pl.when(i > 0)
                def _():
                    finish(k, i - 1, lax.rem(i + 1, 2))
                return carry
            lax.fori_loop(0, 4, step, 0)

        @pl.when(c == 3)
        def _():
            def step(i, carry):
                s = ring_step(i)
                for q in range(2):
                    own[q] = down(s, q)
                for q in range(2):
                    j = tile_of(i, q)
                    slot = 2 * lax.rem(i, 2) + q

                    @pl.when(i < 2)
                    def _():
                        rr_copy(0, slot).wait_send()

                    @pl.when(i >= 2)
                    def _():
                        out_copy(slot, j).wait()
                    o1_copy(j).wait_recv()
                    for k in range(2):
                        rs_wait(k, j)
                    snd[slot] = (own[q] + o1recv[j].astype(F32) + rsrecv[j].astype(F32)).astype(BF16)
                    out_copy(slot, j).start()
                return carry
            lax.fori_loop(0, 4, step, 0)
        return carry

    def rs_wait(k, j):
        remote(icist.at[0, 0, pl.ds(0, HALF), :],
               rsrecv.at[j, pl.ds(k * HALF, HALF), :],
               ici_send.at[0, 0, 0], rs_sem.at[k, j], far).wait_recv()

    lax.fori_loop(0, 4, chunk, 0)

    for i in range(2):
        for q in range(2):
            out_copy(2 * i + q, tile_of(2 + i, q)).wait()
    px().wait_send()
    for k in range(2):
        for p in range(PIECES):
            ag(k, p).wait_send()
            fwd(k, p).wait_send()
        for i in range(4):
            if k == 1:
                rr_copy(k, i).wait_send()
            for r in range(2):
                rs_copy(k, i, r).wait_send()


def solution(mesh):
    def step(x, w_gate, w_up, w_down):
        dma = pltpu.SemaphoreType.DMA
        return pl.pallas_call(
            kernel,
            out_shape=jax.ShapeDtypeStruct((ROWS, D), BF16),
            in_specs=[pl.BlockSpec(memory_space=pl.ANY)] * 4,
            out_specs=pl.BlockSpec(memory_space=pl.ANY),
            scratch_shapes=[
                pltpu.VMEM((3, ROWS, D), BF16),
                pltpu.VMEM((ROWS, F), BF16),
                pltpu.VMEM((3, 2, D, 2 * TA), BF16),
                pltpu.VMEM((4, D, 2 * TA), BF16),
                pltpu.VMEM((D, 2 * REM), BF16),
                pltpu.VMEM((8, ROWS, TB), BF16),
                pltpu.VMEM((8, ROWS, TB), BF16),
                pltpu.VMEM((2, 4, ROWS, TB), BF16),
                pltpu.VMEM((2, 4, ROWS, TB), BF16),
                pltpu.VMEM((8, ROWS, TB), BF16),
                pltpu.VMEM((2, ROWS, TB), F32),
                dma((3, 2, 2)),
                dma((4, 2)),
                dma((2,)),
                dma,
                dma,
                dma,
                dma((2, PIECES)),
                dma((2, PIECES)),
                dma((2, PIECES)),
                dma((2, PIECES)),
                dma((8,)),
                dma((8,)),
                dma((2, 4)),
                dma((2, 4, 2)),
                dma((2, 8)),
                dma((4,)),
            ],
            compiler_params=pltpu.CompilerParams(
                collective_id=0, has_side_effects=True, vmem_limit_bytes=67043328),
            name="mlp_block",
        )(x, w_gate, w_up, w_down)

    return jax.shard_map(
        step,
        mesh=mesh,
        in_specs=(P(("dp", "tp"), None), P(None, "tp"), P(None, "tp"), P("tp", None)),
        out_specs=P(("dp", "tp"), None),
        check_vma=False,
    )
```

```python
import jax
import jax.numpy as jnp
from jax import lax
from jax.experimental import pallas as pl
from jax.experimental.pallas import tpu as pltpu
from jax.sharding import PartitionSpec as P

D = 4096
F = 3200
ROWS = 256
HALF = ROWS // 2
PIECES = 4
PIECE = HALF // PIECES
TA = 256
TB = 512
REM = F - 12 * TA
MESH = pl.DeviceIdType.MESH
VMEM_LIMIT = 67043328 - 9 * 2 ** 18
BF16 = jnp.bfloat16
F32 = jnp.float32


def kernel(x_hbm, wg, wu, wd, y_ref,
           xs, h, wr, wc, wrem, snd, o1recv, rrecv, icist, own0, own1, own2,
           ring_sem, cache_sem, rem_sem, px_send, px_recv, ownx_sem,
           ag_send, ag_recv, fwd_send, fwd_recv, snd_sem, o1_sem, rr_sem,
           ici_send, rs_sem, credit):
    me = lax.axis_index("tp")
    cp = lax.rem(me, 2)
    partner = me + 1 - 2 * cp
    mirror = lax.rem(me + 2, 4)
    far = mirror - cp

    def remote(src, dst, ssem, rsem, dev):
        return pltpu.make_async_remote_copy(
            src_ref=src, dst_ref=dst, send_sem=ssem, recv_sem=rsem,
            device_id={"tp": dev}, device_id_type=MESH)

    def a_copies(t, dst, sems, width):
        cols = pl.ds(t * TA, width)
        return [
            pltpu.make_async_copy(wg.at[:, cols], dst.at[:, pl.ds(0, width)], sems.at[0]),
            pltpu.make_async_copy(wu.at[:, cols], dst.at[:, pl.ds(width, width)], sems.at[1]),
        ]

    def tile_cols(j):
        return pl.ds(pl.multiple_of(j * TB, TB), TB)

    def tile_of(i, q):
        return 2 * i + (1 - cp if q == 0 else cp)

    def ring_a(s, b):
        return [c for q in range(2) for c in a_copies(3 * b + q, wr.at[s, q], ring_sem.at[s, q], TA)]

    def ring_b(s, i):
        out_ = []
        for q in range(2):
            cols = pl.ds(pl.multiple_of(tile_of(i, q) * TB, TB), TB)
            out_.append(pltpu.make_async_copy(wd.at[:, cols], wr.at[s, q, pl.ds(0, F), :], ring_sem.at[s, q, 0]))
        return out_

    def cache(b):
        return a_copies(3 * b + 2, wc.at[b], cache_sem.at[b], TA)

    def rem_copies():
        return a_copies(12, wrem, rem_sem, REM)

    def start(copies):
        for c in copies:
            c.start()

    def wait(copies):
        for c in copies:
            c.wait()

    def px():
        return remote(x_hbm, xs.at[0], px_send, px_recv, partner)

    def ag(k, p):
        return remote(x_hbm.at[pl.ds(k * HALF + p * PIECE, PIECE)],
                      xs.at[1 + k, pl.ds(pl.multiple_of(cp * HALF + p * PIECE, PIECE), PIECE)],
                      ag_send.at[k, p], ag_recv.at[k, p], mirror)

    def fwd(k, p):
        rows = pl.ds(pl.multiple_of(cp * HALF + p * PIECE, PIECE), PIECE)
        return remote(xs.at[1 + k, rows], xs.at[1 + k, rows], fwd_send.at[k, p], fwd_recv.at[k, p], partner)

    def o1_copy(slot, j):
        return remote(snd.at[slot], o1recv.at[j], snd_sem.at[slot], o1_sem.at[j], partner)

    def rr_copy(k, i):
        return remote(snd.at[i], rrecv.at[k, i], snd_sem.at[i], rr_sem.at[k, i], partner)

    def rs_copy(k, i, r):
        j = tile_of(i, 1)
        return remote(icist.at[k, i, pl.ds(r * HALF, HALF), :],
                      xs.at[1, pl.ds(pl.multiple_of(k * HALF, HALF), HALF), tile_cols(j)],
                      ici_send.at[k, i, r], rs_sem.at[k, j], far + r)

    def ownx():
        return pltpu.make_async_copy(x_hbm, xs.at[0], ownx_sem)

    start(ring_a(0, 0))
    start(cache(0))
    start(ring_a(1, 1))
    start(cache(1))

    barrier = pltpu.get_barrier_semaphore()
    for other in (partner, mirror, mirror + 1 - 2 * cp):
        pl.semaphore_signal(barrier, inc=1, device_id={"tp": other}, device_id_type=MESH)
    pl.semaphore_wait(barrier, 3)

    px().start()
    for k in range(2):
        for p in range(PIECES):
            ag(k, p).start()
    start(cache(2))
    start(cache(3))
    start(rem_copies())

    own = (own0, own1, own2)

    def pair_sum(k, i):
        icist[k, i] = (own[i % 3][...] + rrecv[k, i].astype(F32)).astype(BF16)

    def pair_send(k, i):
        for r in range(2):
            rs_copy(k, i, r).start()

    def glu(gu, width):
        g = gu[:, :width]
        return (g * jax.nn.sigmoid(g) * gu[:, width:]).astype(BF16)

    def chunk(c, carry):
        xi = lax.rem(c, 3)

        @pl.when(c == 0)
        def _():
            px().wait_recv()

        @pl.when(c == 1)
        def _():
            ownx().start()
            for p in range(PIECES):
                fwd(0, p).wait_recv()

        @pl.when(c == 2)
        def _():
            for p in range(PIECES):
                fwd(1, p).wait_recv()

        @pl.when(c == 3)
        def _():
            ownx().wait()

        def forward(p):
            for k in range(2):
                @pl.when(c == k)
                def _():
                    ag(k, p).wait_recv()
                    fwd(k, p).start()

        for b in range(4):
            if b == 1:
                forward(0)
                for k in range(2):
                    @pl.when(c == 2 + k)
                    def _():
                        for i in (2, 3):
                            rr_copy(k, i).wait_recv()
                            pair_sum(k, i)
                            pair_send(k, i)
            if b == 3:
                forward(1)
            s = lax.rem(c * 8 + b, 3)
            wait(ring_a(s, b))

            @pl.when(c == 0)
            def _():
                wait(cache(b))
                if b == 3:
                    wait(rem_copies())

            s2 = lax.rem(c * 8 + b + 2, 3)
            start(ring_a(s2, b + 2) if b + 2 < 4 else ring_b(s2, b + 2 - 4))
            for q in range(3):
                w = wr[s, q] if q < 2 else wc[b]
                gu = jnp.dot(xs[xi], w, preferred_element_type=F32)
                h[:, (3 * b + q) * TA:(3 * b + q + 1) * TA] = glu(gu, TA)
            if b == 3:
                gu = jnp.dot(xs[xi], wrem[...], preferred_element_type=F32)
                h[:, 12 * TA:] = glu(gu, REM)
        forward(2)

        @pl.when(c == 1)
        def _():
            for p in range(PIECES):
                fwd(0, p).wait_send()
            for r in range(2):
                pl.semaphore_signal(credit, inc=1, device_id={"tp": far + r}, device_id_type=MESH)

        def ring_step(i):
            g = c * 8 + 4 + i
            s = lax.rem(g, 3)
            wait(ring_b(s, i))
            s2 = lax.rem(g + 2, 3)
            if i < 2:
                start(ring_b(s2, i + 2))
            else:
                @pl.when(c < 3)
                def _():
                    start(ring_a(s2, i - 2))
            return s

        def down(s, q):
            return jnp.dot(h[...], wr[s, q, pl.ds(0, F), :], preferred_element_type=F32)

        @pl.when(c == 0)
        def _():
            for i in range(4):
                if i == 3:
                    forward(3)
                s = ring_step(i)
                slots = [2 * (i % 2) + q for q in range(2)]
                if i >= 2:
                    for q in range(2):
                        o1_copy(slots[q], tile_of(i, q)).wait_send()
                for q in range(2):
                    snd[slots[q]] = down(s, q).astype(BF16)
                for q in range(2):
                    o1_copy(slots[q], tile_of(i, q)).start()

        @pl.when((c == 1) | (c == 2))
        def _():
            k = c - 1
            for i in range(4):
                if i == 3:
                    @pl.when(c == 1)
                    def _():
                        forward(3)
                s = ring_step(i)
                rr_copy(k, i).wait_send()
                if i >= 2:
                    rr_copy(k, i - 2).wait_recv()
                    pair_sum(k, i - 2)
                snd[i] = down(s, 0).astype(BF16)
                own[i % 3][...] = down(s, 1)
                rr_copy(k, i).start()
                if i == 2:
                    @pl.when(c == 1)
                    def _():
                        pl.semaphore_wait(credit, 2)
                if i >= 2:
                    pair_send(k, i - 2)

        @pl.when(c == 3)
        def _():
            def arrive(i):
                for q in range(2):
                    j = tile_of(i, q)
                    o1_copy(0, j).wait_recv()
                    for k in range(2):
                        rs_wait(k, j)

            def total(i, q, mine):
                j = tile_of(i, q)
                cols = tile_cols(j)
                y_ref[:, cols] = (mine + o1recv[j].astype(F32) + xs[1, :, cols].astype(F32)).astype(BF16)

            for i in range(4):
                s = ring_step(i)
                if i < 3:
                    arrive(i)
                    for q in range(2):
                        total(i, q, down(s, q))
                else:
                    for q in range(2):
                        own[q][...] = down(s, q)
                    arrive(i)
                    for q in range(2):
                        total(i, q, own[q][...])
        return carry

    def rs_wait(k, j):
        remote(icist.at[0, 0, pl.ds(0, HALF), :],
               xs.at[1, pl.ds(k * HALF, HALF), tile_cols(j)],
               ici_send.at[0, 0, 0], rs_sem.at[k, j], far).wait_recv()

    lax.fori_loop(0, 4, chunk, 0)

    px().wait_send()
    for k in range(2):
        for p in range(PIECES):
            ag(k, p).wait_send()
            if k == 1:
                fwd(k, p).wait_send()
        for i in range(4):
            if k == 1:
                rr_copy(k, i).wait_send()
            for r in range(2):
                rs_copy(k, i, r).wait_send()


def solution(mesh):
    def step(x, w_gate, w_up, w_down):
        dma = pltpu.SemaphoreType.DMA
        return pl.pallas_call(
            kernel,
            out_shape=pltpu.VMEM((ROWS, D), BF16),
            in_specs=[pl.BlockSpec(memory_space=pl.ANY)] * 4,
            out_specs=pl.BlockSpec(memory_space=pltpu.VMEM),
            scratch_shapes=[
                pltpu.VMEM((3, ROWS, D), BF16),
                pltpu.VMEM((ROWS, F), BF16),
                pltpu.VMEM((3, 2, D, 2 * TA), BF16),
                pltpu.VMEM((4, D, 2 * TA), BF16),
                pltpu.VMEM((D, 2 * REM), BF16),
                pltpu.VMEM((4, ROWS, TB), BF16),
                pltpu.VMEM((8, ROWS, TB), BF16),
                pltpu.VMEM((2, 4, ROWS, TB), BF16),
                pltpu.VMEM((2, 4, ROWS, TB), BF16),
                pltpu.VMEM((ROWS, TB), F32),
                pltpu.VMEM((ROWS, TB), F32),
                pltpu.VMEM((ROWS, TB), F32),
                dma((3, 2, 2)),
                dma((4, 2)),
                dma((2,)),
                dma,
                dma,
                dma,
                dma((2, PIECES)),
                dma((2, PIECES)),
                dma((2, PIECES)),
                dma((2, PIECES)),
                dma((4,)),
                dma((8,)),
                dma((2, 4)),
                dma((2, 4, 2)),
                dma((2, 8)),
                pltpu.SemaphoreType.REGULAR,
            ],
            compiler_params=pltpu.CompilerParams(
                collective_id=0, has_side_effects=True, vmem_limit_bytes=VMEM_LIMIT),
            name="mlp_block",
        )(x, w_gate, w_up, w_down)

    return jax.shard_map(
        step,
        mesh=mesh,
        in_specs=(P(("dp", "tp"), None), P(None, "tp"), P(None, "tp"), P("tp", None)),
        out_specs=P(("dp", "tp"), None),
        check_vma=False,
    )
```

```python
import jax
import jax.numpy as jnp
from jax import lax
from jax.experimental import pallas as pl
from jax.experimental.pallas import tpu as pltpu
from jax.sharding import PartitionSpec as P

D = 4096
F = 3200
ROWS = 256
HALF = ROWS // 2
PIECES = 4
PIECE = HALF // PIECES
TA = 256
TB = 512
REM = F - 12 * TA
MESH = pl.DeviceIdType.MESH
VMEM_LIMIT = 67043328 - 9 * 2 ** 18
BF16 = jnp.bfloat16
F32 = jnp.float32


def kernel(x_hbm, wg, wu, wd, y_ref,
           xs, h, wr, wc, wrem, snd, o1recv, rrecv, icist, own0, own1, own2,
           ring_sem, cache_sem, rem_sem, px_send, px_recv, ownx_sem,
           ag_send, ag_recv, fwd_send, fwd_recv, snd_sem, o1_sem, rr_sem,
           ici_send, rs_sem, credit):
    me = lax.axis_index("tp")
    cp = lax.rem(me, 2)
    partner = me + 1 - 2 * cp
    mirror = lax.rem(me + 2, 4)
    far = mirror - cp

    def remote(src, dst, ssem, rsem, dev):
        return pltpu.make_async_remote_copy(
            src_ref=src, dst_ref=dst, send_sem=ssem, recv_sem=rsem,
            device_id={"tp": dev}, device_id_type=MESH)

    def a_copies(t, dst, sems, width):
        cols = pl.ds(pl.multiple_of(t * TA, TA), width)
        return [
            pltpu.make_async_copy(wg.at[:, cols], dst.at[:, pl.ds(0, width)], sems.at[0]),
            pltpu.make_async_copy(wu.at[:, cols], dst.at[:, pl.ds(width, width)], sems.at[1]),
        ]

    def tile_cols(j):
        return pl.ds(pl.multiple_of(j * TB, TB), TB)

    def tile_of(i, q):
        return 2 * i + (1 - cp if q == 0 else cp)

    def ring_a(s, b):
        return [c for q in range(2) for c in a_copies(3 * b + q, wr.at[s, q], ring_sem.at[s, q], TA)]

    def ring_b(s, i):
        out_ = []
        for q in range(2):
            cols = pl.ds(pl.multiple_of(tile_of(i, q) * TB, TB), TB)
            out_.append(pltpu.make_async_copy(wd.at[:, cols], wr.at[s, q, pl.ds(0, F), :], ring_sem.at[s, q, 0]))
        return out_

    def cache(b):
        return a_copies(3 * b + 2, wc.at[b], cache_sem.at[b], TA)

    def rem_copies():
        return a_copies(12, wrem, rem_sem, REM)

    def start(copies):
        for c in copies:
            c.start()

    def wait(copies):
        for c in copies:
            c.wait()

    def px():
        return remote(x_hbm, xs.at[0], px_send, px_recv, partner)

    def ag(k, p):
        return remote(x_hbm.at[pl.ds(k * HALF + p * PIECE, PIECE)],
                      xs.at[1 + k, pl.ds(pl.multiple_of(cp * HALF + p * PIECE, PIECE), PIECE)],
                      ag_send.at[k, p], ag_recv.at[k, p], mirror)

    def fwd(k, p):
        rows = pl.ds(pl.multiple_of(cp * HALF + p * PIECE, PIECE), PIECE)
        return remote(xs.at[1 + k, rows], xs.at[1 + k, rows], fwd_send.at[k, p], fwd_recv.at[k, p], partner)

    def o1_copy(slot, j):
        return remote(snd.at[slot], o1recv.at[j], snd_sem.at[slot], o1_sem.at[j], partner)

    def rr_copy(k, i):
        return remote(snd.at[i], rrecv.at[k, i], snd_sem.at[i], rr_sem.at[k, i], partner)

    def rs_copy(k, i, r):
        j = tile_of(i, 1)
        return remote(icist.at[k, i, pl.ds(r * HALF, HALF), :],
                      xs.at[1, pl.ds(pl.multiple_of(k * HALF, HALF), HALF), tile_cols(j)],
                      ici_send.at[k, i, r], rs_sem.at[k, j], far + r)

    def ownx():
        return pltpu.make_async_copy(x_hbm, xs.at[0], ownx_sem)

    start(ring_a(0, 0))
    start(cache(0))
    start(ring_a(1, 1))
    start(cache(1))

    barrier = pltpu.get_barrier_semaphore()
    for other in (partner, mirror, mirror + 1 - 2 * cp):
        pl.semaphore_signal(barrier, inc=1, device_id={"tp": other}, device_id_type=MESH)
    pl.semaphore_wait(barrier, 3)

    px().start()
    for k in range(2):
        for p in range(PIECES):
            ag(k, p).start()
    start(cache(2))
    start(cache(3))
    start(rem_copies())

    own = (own0, own1, own2)

    def pair_sum(k, i):
        icist[k, i] = (own[i % 3][...] + rrecv[k, i].astype(F32)).astype(BF16)

    def pair_send(k, i):
        for r in range(2):
            rs_copy(k, i, r).start()

    def glu(gu, width):
        g = gu[:, :width]
        return (g * jax.nn.sigmoid(g) * gu[:, width:]).astype(BF16)

    def chunk(c, carry):
        xi = lax.rem(c, 3)

        @pl.when(c == 0)
        def _():
            px().wait_recv()

        @pl.when(c == 1)
        def _():
            ownx().start()
            for p in range(PIECES):
                fwd(0, p).wait_recv()

        @pl.when(c == 2)
        def _():
            for p in range(PIECES):
                fwd(1, p).wait_recv()

        @pl.when(c == 3)
        def _():
            ownx().wait()

        def forward(p):
            for k in range(2):
                @pl.when(c == k)
                def _():
                    ag(k, p).wait_recv()
                    fwd(k, p).start()

        def tile(t, w, width):
            gu = jnp.dot(xs[xi], w, preferred_element_type=F32)
            h[:, pl.ds(pl.multiple_of(t * TA, TA), width)] = glu(gu, width)

        def block(b, carry):
            @pl.when(b == 1)
            def _():
                forward(0)
                for k in range(2):
                    @pl.when(c == 2 + k)
                    def _():
                        for i in (2, 3):
                            rr_copy(k, i).wait_recv()
                            pair_sum(k, i)
                            pair_send(k, i)
            s = lax.rem(c * 8 + b, 3)
            wait(ring_a(s, b))

            @pl.when(c == 0)
            def _():
                wait(cache(b))
            s2 = lax.rem(c * 8 + b + 2, 3)

            @pl.when(b < 2)
            def _():
                start(ring_a(s2, b + 2))

            @pl.when(b == 2)
            def _():
                start(ring_b(s2, 0))
            for q in range(3):
                tile(3 * b + q, wr[s, q] if q < 2 else wc[b], TA)
            return carry

        lax.fori_loop(0, 3, block, 0)
        forward(1)
        s = lax.rem(c * 8 + 3, 3)
        wait(ring_a(s, 3))

        @pl.when(c == 0)
        def _():
            wait(cache(3))
            wait(rem_copies())
        start(ring_b(lax.rem(c * 8 + 5, 3), 1))
        for q in range(3):
            tile(9 + q, wr[s, q] if q < 2 else wc[3], TA)
        tile(12, wrem[...], REM)
        forward(2)

        @pl.when(c == 1)
        def _():
            for p in range(PIECES):
                fwd(0, p).wait_send()
            for r in range(2):
                pl.semaphore_signal(credit, inc=1, device_id={"tp": far + r}, device_id_type=MESH)

        def ring_step(i):
            g = c * 8 + 4 + i
            s = lax.rem(g, 3)
            wait(ring_b(s, i))
            s2 = lax.rem(g + 2, 3)
            if i < 2:
                start(ring_b(s2, i + 2))
            else:
                @pl.when(c < 3)
                def _():
                    start(ring_a(s2, i - 2))
            return s

        def down(s, q):
            return jnp.dot(h[...], wr[s, q, pl.ds(0, F), :], preferred_element_type=F32)

        @pl.when(c == 0)
        def _():
            for i in range(4):
                if i == 3:
                    forward(3)
                s = ring_step(i)
                slots = [2 * (i % 2) + q for q in range(2)]
                if i >= 2:
                    for q in range(2):
                        o1_copy(slots[q], tile_of(i, q)).wait_send()
                for q in range(2):
                    snd[slots[q]] = down(s, q).astype(BF16)
                for q in range(2):
                    o1_copy(slots[q], tile_of(i, q)).start()

        @pl.when((c == 1) | (c == 2))
        def _():
            k = c - 1
            for i in range(4):
                if i == 3:
                    @pl.when(c == 1)
                    def _():
                        forward(3)
                s = ring_step(i)
                rr_copy(k, i).wait_send()
                if i >= 2:
                    rr_copy(k, i - 2).wait_recv()
                    pair_sum(k, i - 2)
                snd[i] = down(s, 0).astype(BF16)
                own[i % 3][...] = down(s, 1)
                rr_copy(k, i).start()
                if i == 2:
                    @pl.when(c == 1)
                    def _():
                        pl.semaphore_wait(credit, 2)
                if i >= 2:
                    pair_send(k, i - 2)

        @pl.when(c == 3)
        def _():
            def arrive(i):
                for q in range(2):
                    j = tile_of(i, q)
                    o1_copy(0, j).wait_recv()
                    for k in range(2):
                        rs_wait(k, j)

            def total(i, q, mine):
                j = tile_of(i, q)
                cols = tile_cols(j)
                y_ref[:, cols] = (mine + o1recv[j].astype(F32) + xs[1, :, cols].astype(F32)).astype(BF16)

            for i in range(4):
                s = ring_step(i)
                if i < 3:
                    arrive(i)
                    for q in range(2):
                        total(i, q, down(s, q))
                else:
                    for q in range(2):
                        own[q][...] = down(s, q)
                    arrive(i)
                    for q in range(2):
                        total(i, q, own[q][...])
        return carry

    def rs_wait(k, j):
        remote(icist.at[0, 0, pl.ds(0, HALF), :],
               xs.at[1, pl.ds(k * HALF, HALF), tile_cols(j)],
               ici_send.at[0, 0, 0], rs_sem.at[k, j], far).wait_recv()

    lax.fori_loop(0, 4, chunk, 0)

    px().wait_send()
    for k in range(2):
        for p in range(PIECES):
            ag(k, p).wait_send()
            if k == 1:
                fwd(k, p).wait_send()
        for i in range(4):
            if k == 1:
                rr_copy(k, i).wait_send()
            for r in range(2):
                rs_copy(k, i, r).wait_send()


def solution(mesh):
    def step(x, w_gate, w_up, w_down):
        dma = pltpu.SemaphoreType.DMA
        return pl.pallas_call(
            kernel,
            out_shape=pltpu.VMEM((ROWS, D), BF16),
            in_specs=[pl.BlockSpec(memory_space=pl.ANY)] * 4,
            out_specs=pl.BlockSpec(memory_space=pltpu.VMEM),
            scratch_shapes=[
                pltpu.VMEM((3, ROWS, D), BF16),
                pltpu.VMEM((ROWS, F), BF16),
                pltpu.VMEM((3, 2, D, 2 * TA), BF16),
                pltpu.VMEM((4, D, 2 * TA), BF16),
                pltpu.VMEM((D, 2 * REM), BF16),
                pltpu.VMEM((4, ROWS, TB), BF16),
                pltpu.VMEM((8, ROWS, TB), BF16),
                pltpu.VMEM((2, 4, ROWS, TB), BF16),
                pltpu.VMEM((2, 4, ROWS, TB), BF16),
                pltpu.VMEM((ROWS, TB), F32),
                pltpu.VMEM((ROWS, TB), F32),
                pltpu.VMEM((ROWS, TB), F32),
                dma((3, 2, 2)),
                dma((4, 2)),
                dma((2,)),
                dma,
                dma,
                dma,
                dma((2, PIECES)),
                dma((2, PIECES)),
                dma((2, PIECES)),
                dma((2, PIECES)),
                dma((4,)),
                dma((8,)),
                dma((2, 4)),
                dma((2, 4, 2)),
                dma((2, 8)),
                pltpu.SemaphoreType.REGULAR,
            ],
            compiler_params=pltpu.CompilerParams(
                collective_id=0, has_side_effects=True, vmem_limit_bytes=VMEM_LIMIT),
            name="mlp_block",
        )(x, w_gate, w_up, w_down)

    return jax.shard_map(
        step,
        mesh=mesh,
        in_specs=(P(("dp", "tp"), None), P(None, "tp"), P(None, "tp"), P("tp", None)),
        out_specs=P(("dp", "tp"), None),
        check_vma=False,
    )
```

```python
import jax
import jax.numpy as jnp
from jax import lax
from jax.experimental import pallas as pl
from jax.experimental.pallas import tpu as pltpu
from jax.sharding import PartitionSpec as P

D = 4096
F = 3200
ROWS = 256
HALF = ROWS // 2
PIECES = 4
PIECE = HALF // PIECES
TA = 256
TB = 512
REM = F - 12 * TA
MESH = pl.DeviceIdType.MESH
VMEM_LIMIT = 67043328 - 9 * 2 ** 18
BF16 = jnp.bfloat16
F32 = jnp.float32


def kernel(x_hbm, wg, wu, wd, y_ref,
           xs, h, hown, wr, wc, wrem, snd, o1recv, rrecv, icist, own0, own1,
           ring_sem, cache_sem, rem_sem, px_send, px_recv, ownx_sem,
           ag_send, ag_recv, fwd_send, fwd_recv, snd_sem, o1_sem, rr_sem,
           ici_send, rs_sem, credit, free):
    me = lax.axis_index("tp")
    cp = lax.rem(me, 2)
    partner = me + 1 - 2 * cp
    mirror = lax.rem(me + 2, 4)
    far = mirror - cp

    def remote(src, dst, ssem, rsem, dev):
        return pltpu.make_async_remote_copy(
            src_ref=src, dst_ref=dst, send_sem=ssem, recv_sem=rsem,
            device_id={"tp": dev}, device_id_type=MESH)

    def a_copies(t, dst, sems, width):
        cols = pl.ds(pl.multiple_of(t * TA, TA), width)
        return [
            pltpu.make_async_copy(wg.at[:, cols], dst.at[:, pl.ds(0, width)], sems.at[0]),
            pltpu.make_async_copy(wu.at[:, cols], dst.at[:, pl.ds(width, width)], sems.at[1]),
        ]

    def tile_cols(j):
        return pl.ds(pl.multiple_of(j * TB, TB), TB)

    def tile_of(i, q):
        return 2 * i + (1 - cp if q == 0 else cp)

    def down_tile(c, i, q):
        last = c // 3
        other = 2 * (2 * (i // 2) + q) + (1 - cp if i % 2 == 0 else cp)
        return last * tile_of(i, q) + (1 - last) * other

    def ring_a(s, b):
        return [c for q in range(2) for c in a_copies(3 * b + q, wr.at[s, q], ring_sem.at[s, q], TA)]

    def ring_b(c, s, i):
        out_ = []
        for q in range(2):
            cols = tile_cols(down_tile(c, i, q))
            out_.append(pltpu.make_async_copy(wd.at[:, cols], wr.at[s, q, pl.ds(0, F), :], ring_sem.at[s, q, 0]))
        return out_

    def cache(b):
        return a_copies(3 * b + 2, wc.at[b], cache_sem.at[b], TA)

    def rem_copies():
        return a_copies(12, wrem, rem_sem, REM)

    def start(copies):
        for c in copies:
            c.start(priority=1)

    def wait(copies):
        for c in copies:
            c.wait()

    def px():
        return remote(x_hbm, xs.at[0], px_send, px_recv, partner)

    def ag(k, p):
        return remote(x_hbm.at[pl.ds(k * HALF + p * PIECE, PIECE)],
                      xs.at[1 + k, pl.ds(pl.multiple_of(cp * HALF + p * PIECE, PIECE), PIECE)],
                      ag_send.at[k, p], ag_recv.at[k, p], mirror)

    def fwd(k, p):
        rows = pl.ds(pl.multiple_of(cp * HALF + p * PIECE, PIECE), PIECE)
        return remote(xs.at[1 + k, rows], xs.at[1 + k, rows], fwd_send.at[k, p], fwd_recv.at[k, p], partner)

    def o1_copy(slot, j):
        return remote(snd.at[slot], o1recv.at[j], snd_sem.at[slot], o1_sem.at[j], partner)

    def rr_copy(k, i):
        return remote(snd.at[i], rrecv.at[k, i], snd_sem.at[i], rr_sem.at[k, i], partner)

    def rs_copy(k, i, r):
        j = tile_of(i, 1)
        return remote(icist.at[k, i, pl.ds(r * HALF, HALF), :],
                      xs.at[1, pl.ds(pl.multiple_of(k * HALF, HALF), HALF), tile_cols(j)],
                      ici_send.at[k, i, r], rs_sem.at[k, j], far + r)

    def ownx(slot):
        return pltpu.make_async_copy(x_hbm, xs.at[slot], ownx_sem)

    ownx(2).start()
    start(ring_a(0, 0))
    start(cache(0))

    barrier = pltpu.get_barrier_semaphore()
    for other in (partner, mirror, mirror + 1 - 2 * cp):
        pl.semaphore_signal(barrier, inc=1, device_id={"tp": other}, device_id_type=MESH)
    pl.semaphore_wait(barrier, 3)

    px().start()
    for p in range(PIECES):
        ag(0, p).start()

    own = (own0, own1)

    def pair_sum(k, i):
        icist[k, i] = (own[i % 2][...] + rrecv[k, i].astype(F32)).astype(BF16)

    def pair_send(k, i):
        for r in range(2):
            rs_copy(k, i, r).start()

    def glu(gu, width):
        g = gu[:, :width]
        return (g * jax.nn.sigmoid(g) * gu[:, width:]).astype(BF16)

    first = ring_a(0, 0)
    ownx(2).wait()
    for q in range(3):
        wait(first[2 * q:2 * q + 2] if q < 2 else cache(0))
        start((ring_a(1, 1), cache(1), ring_a(2, 2))[q])
        gu = jnp.dot(xs[2], wr[0, q] if q < 2 else wc[0], preferred_element_type=F32)
        hown[:, q * TA:(q + 1) * TA] = glu(gu, TA)
    pl.semaphore_signal(free, inc=1, device_id={"tp": mirror}, device_id_type=MESH)

    def chunk(c, carry):
        xi = lax.rem(c, 3)
        skip = c // 3

        @pl.when(c == 0)
        def _():
            px().wait_recv()

        @pl.when(c == 1)
        def _():
            ownx(0).start()
            for p in range(PIECES):
                fwd(0, p).wait_recv()

        @pl.when(c == 2)
        def _():
            for p in range(PIECES):
                fwd(1, p).wait_recv()

        @pl.when(c == 3)
        def _():
            ownx(0).wait()
            h[:, :3 * TA] = hown[...]

        def forward(p):
            for k in range(2):
                @pl.when(c == k)
                def _():
                    ag(k, p).wait_recv()
                    fwd(k, p).start()

        def tile(t, w, width):
            gu = jnp.dot(xs[xi], w, preferred_element_type=F32)
            h[:, pl.ds(pl.multiple_of(t * TA, TA), width)] = glu(gu, width)

        def slot_of(n):
            return lax.rem(c * 8 + n - skip, 3)

        def block(b, carry):
            @pl.when(b == 1)
            def _():
                forward(0)

            @pl.when((b == 1) & (c == 0))
            def _():
                pl.semaphore_wait(free, 1)
                for p in range(PIECES):
                    ag(1, p).start()
            s = slot_of(b)

            @pl.when(c + b > 0)
            def _():
                wait(ring_a(s, b))

            @pl.when((c == 0) & (b > 0))
            def _():
                wait(cache(b))

            @pl.when((c == 0) & (b < 2))
            def _():
                start(cache(b + 2))

            @pl.when((c == 0) & (b == 1))
            def _():
                start(rem_copies())
            s2 = slot_of(b + 2)

            @pl.when((b < 2) & (c + b > 0))
            def _():
                start(ring_a(s2, b + 2))

            @pl.when(b == 2)
            def _():
                start(ring_b(c, s2, 0))
            for q in range(3):
                tile(3 * b + q, wr[s, q] if q < 2 else wc[b], TA)
            return carry

        lax.fori_loop(skip, 3, block, 0)
        forward(1)
        s = slot_of(3)
        wait(ring_a(s, 3))

        @pl.when(c == 0)
        def _():
            wait(cache(3))
            wait(rem_copies())
        start(ring_b(c, slot_of(5), 1))
        for q in range(3):
            tile(9 + q, wr[s, q] if q < 2 else wc[3], TA)
        tile(12, wrem[...], REM)
        forward(2)

        @pl.when(c == 1)
        def _():
            for p in range(PIECES):
                fwd(0, p).wait_send()
            for r in range(2):
                pl.semaphore_signal(credit, inc=1, device_id={"tp": far + r}, device_id_type=MESH)

        def ring_step(i):
            s = slot_of(4 + i)
            wait(ring_b(c, s, i))
            s2 = slot_of(6 + i)
            if i < 2:
                start(ring_b(c, s2, i + 2))
            else:
                @pl.when(c < 3)
                def _():
                    start(ring_a(s2, i - 2 + c // 2))
            return s

        def down(s, q):
            return jnp.dot(h[...], wr[s, q, pl.ds(0, F), :], preferred_element_type=F32)

        @pl.when(c == 0)
        def _():
            for i in range(4):
                if i == 3:
                    forward(3)
                s = ring_step(i)
                slots = [2 * (i % 2) + q for q in range(2)]
                if i >= 2:
                    for q in range(2):
                        o1_copy(slots[q], down_tile(c, i, q)).wait_send()
                for q in range(2):
                    snd[slots[q]] = down(s, q).astype(BF16)
                for q in range(2):
                    o1_copy(slots[q], down_tile(c, i, q)).start()

        @pl.when((c == 1) | (c == 2))
        def _():
            k = c - 1
            for i in range(4):
                if i == 3:
                    @pl.when(c == 1)
                    def _():
                        forward(3)
                s = ring_step(i)
                pairs = (2 * (i // 2), 2 * (i // 2) + 1)
                if i % 2 == 0:
                    for p in pairs:
                        rr_copy(k, p).wait_send()
                    for q, p in enumerate(pairs):
                        snd[p] = down(s, q).astype(BF16)
                    for p in pairs:
                        rr_copy(k, p).start()
                else:
                    for q in range(2):
                        own[q][...] = down(s, q)
                    if i == 1:
                        @pl.when(c == 1)
                        def _():
                            pl.semaphore_wait(credit, 2)
                    for p in pairs:
                        rr_copy(k, p).wait_recv()
                        pair_sum(k, p)
                        pair_send(k, p)

        @pl.when(c == 3)
        def _():
            def arrive(i):
                for q in range(2):
                    j = tile_of(i, q)
                    o1_copy(0, j).wait_recv()
                    for k in range(2):
                        rs_wait(k, j)

            def total(i, q, mine):
                j = tile_of(i, q)
                cols = tile_cols(j)
                y_ref[:, cols] = (mine + o1recv[j].astype(F32) + xs[1, :, cols].astype(F32)).astype(BF16)

            for i in range(4):
                s = ring_step(i)
                if i < 3:
                    arrive(i)
                    for q in range(2):
                        total(i, q, down(s, q))
                else:
                    for q in range(2):
                        own[q][...] = down(s, q)
                    arrive(i)
                    for q in range(2):
                        total(i, q, own[q][...])
        return carry

    def rs_wait(k, j):
        remote(icist.at[0, 0, pl.ds(0, HALF), :],
               xs.at[1, pl.ds(k * HALF, HALF), tile_cols(j)],
               ici_send.at[0, 0, 0], rs_sem.at[k, j], far).wait_recv()

    lax.fori_loop(0, 4, chunk, 0)

    px().wait_send()
    for k in range(2):
        for p in range(PIECES):
            ag(k, p).wait_send()
            if k == 1:
                fwd(k, p).wait_send()
        for i in range(4):
            if k == 1:
                rr_copy(k, i).wait_send()
            for r in range(2):
                rs_copy(k, i, r).wait_send()


def solution(mesh):
    def step(x, w_gate, w_up, w_down):
        dma = pltpu.SemaphoreType.DMA
        return pl.pallas_call(
            kernel,
            out_shape=pltpu.VMEM((ROWS, D), BF16),
            in_specs=[pl.BlockSpec(memory_space=pl.ANY)] * 4,
            out_specs=pl.BlockSpec(memory_space=pltpu.VMEM),
            scratch_shapes=[
                pltpu.VMEM((3, ROWS, D), BF16),
                pltpu.VMEM((ROWS, F), BF16),
                pltpu.VMEM((ROWS, 3 * TA), BF16),
                pltpu.VMEM((3, 2, D, 2 * TA), BF16),
                pltpu.VMEM((4, D, 2 * TA), BF16),
                pltpu.VMEM((D, 2 * REM), BF16),
                pltpu.VMEM((4, ROWS, TB), BF16),
                pltpu.VMEM((8, ROWS, TB), BF16),
                pltpu.VMEM((2, 4, ROWS, TB), BF16),
                pltpu.VMEM((2, 4, ROWS, TB), BF16),
                pltpu.VMEM((ROWS, TB), F32),
                pltpu.VMEM((ROWS, TB), F32),
                dma((3, 2, 2)),
                dma((4, 2)),
                dma((2,)),
                dma,
                dma,
                dma,
                dma((2, PIECES)),
                dma((2, PIECES)),
                dma((2, PIECES)),
                dma((2, PIECES)),
                dma((4,)),
                dma((8,)),
                dma((2, 4)),
                dma((2, 4, 2)),
                dma((2, 8)),
                pltpu.SemaphoreType.REGULAR,
                pltpu.SemaphoreType.REGULAR,
            ],
            compiler_params=pltpu.CompilerParams(
                collective_id=0, has_side_effects=True, vmem_limit_bytes=VMEM_LIMIT),
            name="mlp_block",
        )(x, w_gate, w_up, w_down)

    return jax.shard_map(
        step,
        mesh=mesh,
        in_specs=(P(("dp", "tp"), None), P(None, "tp"), P(None, "tp"), P("tp", None)),
        out_specs=P(("dp", "tp"), None),
        check_vma=False,
    )
```

```python
import jax
import jax.numpy as jnp
from jax import lax
from jax.experimental import pallas as pl
from jax.experimental.pallas import tpu as pltpu
from jax.sharding import PartitionSpec as P

D = 4096
F = 3200
ROWS = 256
HALF = ROWS // 2
PIECES = 4
PIECE = HALF // PIECES
TA = 256
TB = 512
REM = F - 12 * TA
MESH = pl.DeviceIdType.MESH
VMEM_LIMIT = 67043328 - 9 * 2 ** 18
BF16 = jnp.bfloat16
F32 = jnp.float32


def kernel(x_hbm, wg, wu, wd, y_ref,
           xs, h, hown, wr, wc, wrem, snd, o1recv, rrecv, icist, own0, own1,
           ring_sem, cache_sem, rem_sem, px_send, px_recv, ownx_sem,
           ag_send, ag_recv, fwd_send, fwd_recv, snd_sem, o1_sem, rr_sem,
           ici_send, rs_sem, credit, free):
    me = lax.axis_index("tp")
    cp = lax.rem(me, 2)
    partner = me + 1 - 2 * cp
    mirror = lax.rem(me + 2, 4)
    far = mirror - cp

    def remote(src, dst, ssem, rsem, dev):
        return pltpu.make_async_remote_copy(
            src_ref=src, dst_ref=dst, send_sem=ssem, recv_sem=rsem,
            device_id={"tp": dev}, device_id_type=MESH)

    def a_copies(t, dst, sems, width):
        cols = pl.ds(pl.multiple_of(t * TA, TA), width)
        return [
            pltpu.make_async_copy(wg.at[:, cols], dst.at[:, pl.ds(0, width)], sems.at[0]),
            pltpu.make_async_copy(wu.at[:, cols], dst.at[:, pl.ds(width, width)], sems.at[1]),
        ]

    def tile_cols(j):
        return pl.ds(pl.multiple_of(j * TB, TB), TB)

    def tile_of(i, q):
        return 2 * i + (1 - cp if q == 0 else cp)

    def down_tile(c, i, q):
        last = c // 3
        other = 2 * (2 * (i // 2) + q) + (1 - cp if i % 2 == 0 else cp)
        return last * tile_of(i, q) + (1 - last) * other

    def ring_a(s, b):
        return [c for q in range(2) for c in a_copies(3 * b + q, wr.at[s, q], ring_sem.at[s, q], TA)]

    def ring_b(c, s, i):
        out_ = []
        for q in range(2):
            cols = tile_cols(down_tile(c, i, q))
            out_.append(pltpu.make_async_copy(wd.at[:, cols], wr.at[s, q, pl.ds(0, F), :], ring_sem.at[s, q, 0]))
        return out_

    def cache(b):
        return a_copies(3 * b + 2, wc.at[b], cache_sem.at[b], TA)

    def rem_copies():
        return a_copies(12, wrem, rem_sem, REM)

    def start(copies):
        for c in copies:
            c.start(priority=1)

    def wait(copies):
        for c in copies:
            c.wait()

    def px():
        return remote(x_hbm, xs.at[0], px_send, px_recv, partner)

    def ag(k, p):
        return remote(x_hbm.at[pl.ds(k * HALF + p * PIECE, PIECE)],
                      xs.at[1 + k, pl.ds(pl.multiple_of(cp * HALF + p * PIECE, PIECE), PIECE)],
                      ag_send.at[k, p], ag_recv.at[k, p], mirror)

    def fwd(k, p):
        rows = pl.ds(pl.multiple_of(cp * HALF + p * PIECE, PIECE), PIECE)
        return remote(xs.at[1 + k, rows], xs.at[1 + k, rows], fwd_send.at[k, p], fwd_recv.at[k, p], partner)

    def o1_copy(slot, j):
        return remote(snd.at[slot], o1recv.at[j], snd_sem.at[slot], o1_sem.at[j], partner)

    def rr_copy(k, i):
        return remote(snd.at[i], rrecv.at[k, i], snd_sem.at[i], rr_sem.at[k, i], partner)

    def rs_copy(k, i, r):
        j = tile_of(i, 1)
        return remote(icist.at[k, i, pl.ds(r * HALF, HALF), :],
                      xs.at[1, pl.ds(pl.multiple_of(k * HALF, HALF), HALF), tile_cols(j)],
                      ici_send.at[k, i, r], rs_sem.at[k, j], far + r)

    def ownx(slot):
        return pltpu.make_async_copy(x_hbm, xs.at[slot], ownx_sem)

    barrier = pltpu.get_barrier_semaphore()
    for other in (partner, mirror, mirror + 1 - 2 * cp):
        pl.semaphore_signal(barrier, inc=1, device_id={"tp": other}, device_id_type=MESH)

    ownx(2).start()
    start(ring_a(0, 0))
    pl.semaphore_wait(barrier, 3)
    for p in range(PIECES):
        ag(0, p).start()
    px().start()
    start(cache(0))


    own = (own0, own1)

    def pair_sum(k, i):
        icist[k, i] = (own[i % 2][...] + rrecv[k, i].astype(F32)).astype(BF16)

    def pair_send(k, i):
        for r in range(2):
            rs_copy(k, i, r).start()

    def glu(gu, width):
        g = gu[:, :width]
        return (g * jax.nn.sigmoid(g) * gu[:, width:]).astype(BF16)

    first = ring_a(0, 0)
    ownx(2).wait()
    for q in range(3):
        wait(first[2 * q:2 * q + 2] if q < 2 else cache(0))
        start((ring_a(1, 1), cache(1), ring_a(2, 2))[q])
        gu = jnp.dot(xs[2], wr[0, q] if q < 2 else wc[0], preferred_element_type=F32)
        hown[:, q * TA:(q + 1) * TA] = glu(gu, TA)
    pl.semaphore_signal(free, inc=1, device_id={"tp": mirror}, device_id_type=MESH)

    def chunk(c, carry):
        xi = lax.rem(c, 3)
        skip = c // 3

        @pl.when(c == 0)
        def _():
            px().wait_recv()

        @pl.when(c == 1)
        def _():
            ownx(0).start()
            for p in range(PIECES):
                fwd(0, p).wait_recv()

        @pl.when(c == 2)
        def _():
            for p in range(PIECES):
                fwd(1, p).wait_recv()

        @pl.when(c == 3)
        def _():
            ownx(0).wait()
            h[:, :3 * TA] = hown[...]

        def forward(p):
            for k in range(2):
                @pl.when(c == k)
                def _():
                    ag(k, p).wait_recv()
                    fwd(k, p).start()

        def tile(t, w, width):
            gu = jnp.dot(xs[xi], w, preferred_element_type=F32)
            h[:, pl.ds(pl.multiple_of(t * TA, TA), width)] = glu(gu, width)

        def slot_of(n):
            return lax.rem(c * 8 + n - skip, 3)

        def block(b, carry):
            @pl.when(b == 1)
            def _():
                forward(0)

            @pl.when((b == 1) & (c == 0))
            def _():
                pl.semaphore_wait(free, 1)
                for p in range(PIECES):
                    ag(1, p).start()
            s = slot_of(b)

            @pl.when(c + b > 0)
            def _():
                wait(ring_a(s, b))

            @pl.when((c == 0) & (b > 0))
            def _():
                wait(cache(b))

            @pl.when((c == 0) & (b < 2))
            def _():
                start(cache(b + 2))

            @pl.when((c == 0) & (b == 1))
            def _():
                start(rem_copies())
            s2 = slot_of(b + 2)

            @pl.when((b < 2) & (c + b > 0))
            def _():
                start(ring_a(s2, b + 2))

            @pl.when(b == 2)
            def _():
                start(ring_b(c, s2, 0))
            for q in range(3):
                tile(3 * b + q, wr[s, q] if q < 2 else wc[b], TA)
            return carry

        lax.fori_loop(skip, 3, block, 0)
        forward(1)
        s = slot_of(3)
        wait(ring_a(s, 3))

        @pl.when(c == 0)
        def _():
            wait(cache(3))
            wait(rem_copies())
        start(ring_b(c, slot_of(5), 1))
        for q in range(3):
            tile(9 + q, wr[s, q] if q < 2 else wc[3], TA)
        tile(12, wrem[...], REM)
        forward(2)

        @pl.when(c == 1)
        def _():
            for p in range(PIECES):
                fwd(0, p).wait_send()
            for r in range(2):
                pl.semaphore_signal(credit, inc=1, device_id={"tp": far + r}, device_id_type=MESH)

        def ring_step(i):
            s = slot_of(4 + i)
            wait(ring_b(c, s, i))
            s2 = slot_of(6 + i)
            if i < 2:
                start(ring_b(c, s2, i + 2))
            else:
                @pl.when(c < 3)
                def _():
                    start(ring_a(s2, i - 2 + c // 2))
            return s

        def down(s, q):
            return jnp.dot(h[...], wr[s, q, pl.ds(0, F), :], preferred_element_type=F32)

        @pl.when(c == 0)
        def _():
            for i in range(4):
                if i == 3:
                    forward(3)
                s = ring_step(i)
                slots = [2 * (i % 2) + q for q in range(2)]
                if i >= 2:
                    for q in range(2):
                        o1_copy(slots[q], down_tile(c, i, q)).wait_send()
                for q in range(2):
                    snd[slots[q]] = down(s, q).astype(BF16)
                for q in range(2):
                    o1_copy(slots[q], down_tile(c, i, q)).start()

        @pl.when((c == 1) | (c == 2))
        def _():
            k = c - 1
            for i in range(4):
                if i == 3:
                    @pl.when(c == 1)
                    def _():
                        forward(3)
                s = ring_step(i)
                pairs = (2 * (i // 2), 2 * (i // 2) + 1)
                if i % 2 == 0:
                    for p in pairs:
                        rr_copy(k, p).wait_send()
                    for q, p in enumerate(pairs):
                        snd[p] = down(s, q).astype(BF16)
                    for p in pairs:
                        rr_copy(k, p).start()
                else:
                    for q in range(2):
                        own[q][...] = down(s, q)
                    if i == 1:
                        @pl.when(c == 1)
                        def _():
                            pl.semaphore_wait(credit, 2)
                    for p in pairs:
                        rr_copy(k, p).wait_recv()
                        pair_sum(k, p)
                        pair_send(k, p)

        @pl.when(c == 3)
        def _():
            def arrive(i):
                for q in range(2):
                    j = tile_of(i, q)
                    o1_copy(0, j).wait_recv()
                    for k in range(2):
                        rs_wait(k, j)

            def total(i, q, mine):
                j = tile_of(i, q)
                cols = tile_cols(j)
                y_ref[:, cols] = (mine + o1recv[j].astype(F32) + xs[1, :, cols].astype(F32)).astype(BF16)

            for i in range(4):
                s = ring_step(i)
                if i < 3:
                    arrive(i)
                    for q in range(2):
                        total(i, q, down(s, q))
                else:
                    for q in range(2):
                        own[q][...] = down(s, q)
                    arrive(i)
                    for q in range(2):
                        total(i, q, own[q][...])
        return carry

    def rs_wait(k, j):
        remote(icist.at[0, 0, pl.ds(0, HALF), :],
               xs.at[1, pl.ds(k * HALF, HALF), tile_cols(j)],
               ici_send.at[0, 0, 0], rs_sem.at[k, j], far).wait_recv()

    lax.fori_loop(0, 4, chunk, 0)

    px().wait_send()
    for k in range(2):
        for p in range(PIECES):
            ag(k, p).wait_send()
            if k == 1:
                fwd(k, p).wait_send()
        for i in range(4):
            if k == 1:
                rr_copy(k, i).wait_send()
            for r in range(2):
                rs_copy(k, i, r).wait_send()


def solution(mesh):
    def step(x, w_gate, w_up, w_down):
        dma = pltpu.SemaphoreType.DMA
        return pl.pallas_call(
            kernel,
            out_shape=pltpu.VMEM((ROWS, D), BF16),
            in_specs=[pl.BlockSpec(memory_space=pl.ANY)] * 4,
            out_specs=pl.BlockSpec(memory_space=pltpu.VMEM),
            scratch_shapes=[
                pltpu.VMEM((3, ROWS, D), BF16),
                pltpu.VMEM((ROWS, F), BF16),
                pltpu.VMEM((ROWS, 3 * TA), BF16),
                pltpu.VMEM((3, 2, D, 2 * TA), BF16),
                pltpu.VMEM((4, D, 2 * TA), BF16),
                pltpu.VMEM((D, 2 * REM), BF16),
                pltpu.VMEM((4, ROWS, TB), BF16),
                pltpu.VMEM((8, ROWS, TB), BF16),
                pltpu.VMEM((2, 4, ROWS, TB), BF16),
                pltpu.VMEM((2, 4, ROWS, TB), BF16),
                pltpu.VMEM((ROWS, TB), F32),
                pltpu.VMEM((ROWS, TB), F32),
                dma((3, 2, 2)),
                dma((4, 2)),
                dma((2,)),
                dma,
                dma,
                dma,
                dma((2, PIECES)),
                dma((2, PIECES)),
                dma((2, PIECES)),
                dma((2, PIECES)),
                dma((4,)),
                dma((8,)),
                dma((2, 4)),
                dma((2, 4, 2)),
                dma((2, 8)),
                pltpu.SemaphoreType.REGULAR,
                pltpu.SemaphoreType.REGULAR,
            ],
            compiler_params=pltpu.CompilerParams(
                collective_id=0, has_side_effects=True, vmem_limit_bytes=VMEM_LIMIT),
            name="mlp_block",
        )(x, w_gate, w_up, w_down)

    return jax.shard_map(
        step,
        mesh=mesh,
        in_specs=(P(("dp", "tp"), None), P(None, "tp"), P(None, "tp"), P("tp", None)),
        out_specs=P(("dp", "tp"), None),
        check_vma=False,
    )
```
